32 devices in a mesh: seq: 16 (over z, x, core), head: 2 (over y).
Axes of the slice: x: 2, y: 2, z: 4, core: 2. Of those that a mesh axis runs over, the one named last changes fastest.
Arguments:
- query: bfloat16 [8192, 1024], P('seq', 'head'), may hold values from -6 to 6
- key_rows: bfloat16 [8192, 128], P('seq'), may hold values from -6 to 6
- value_rows: bfloat16 [8192, 128], P('seq'), may hold values from -6 to 6
- output: bfloat16 [8192, 1024], P('seq', 'head'), may hold values from -1.5 to 1.5
- grad_output: bfloat16 [8192, 1024], P('seq', 'head'), may hold values from -144 to 144
- log_norm: float32 [8, 8192], P('head', 'seq'), may hold values from 0.5 to 12
- stripe: int32 [16], replicated, may hold values from 0 to 15, each once
Outputs:
- grad_query: bfloat16 [8192, 1024], P('seq', 'head')
- grad_key: bfloat16 [8192, 128], P(('seq', 'head'))
- grad_value: bfloat16 [8192, 128], P(('seq', 'head'))
The draws below stay inside these ranges and needn't reach their ends.
Inputs may be any that keep to these rules, and one draw needn't show every extreme that they name: stripe is a permutation of 0 to 15.
All inputs are finite; a program needn't handle non-finite values.
Results may differ from the reference program's by a relative error of at most 0.0051.
Values may be sent and summed in bfloat16 or wider, within the bound.
A program may use at most 192 MiB of HBM per device.

```python
import jax
import jax.numpy as jnp
from jax import lax

DH = 128
QH = 8
WINDOW = 8
S_DEV = 512
LEN = 8192
N_SEQ = 16


def draw_log_norm(key, part):
    local_row = (jnp.arange(LEN) % S_DEV).astype(jnp.float32)
    counts = WINDOW * (local_row + 0.5)
    base_level = jnp.log(counts) + 0.5
    jitter = jax.random.normal(key, (QH, LEN), jnp.float32) * 0.2
    return jnp.clip(base_level[None, :] + jitter, 0.5, 12.0).astype(jnp.float32)


def shard_levels(stream_key, shape, cuts, least, top_value):
    def one(position, parts):
        steps = jax.random.uniform(jax.random.fold_in(jax.random.fold_in(stream_key, 6), position), (parts,), jnp.float32, least / len(cuts), top_value / len(cuts))
        return jnp.repeat(jnp.exp(steps), shape[position] // parts).reshape((-1,) + (1,) * (len(shape) - position - 1))

    loudness = one(*cuts[0])
    for cut in cuts[1:]:
        loudness = loudness * one(*cut)
    return loudness


def scatter_about(rng, shape, deviation, bound, split=(), held_as=jnp.bfloat16):
    entries = jax.random.normal(rng, shape, jnp.float32) * deviation
    if len(split) > 0:
        entries = shard_levels(rng, shape, split, -0.22, 0.18) * entries
    return jnp.clip(entries, min=-bound, max=bound).astype(held_as)


def setup_inputs(seed: int = 0) -> dict:
    keys = jax.random.split(jax.random.key(seed), 8)
    query = scatter_about(keys[0], (LEN, QH * DH), 1.0, 6.0, ((0, 16), (1, 2)))
    key_rows = scatter_about(keys[1], (LEN, DH), 1.0, 6.0, ((0, 16),))
    value_rows = scatter_about(keys[2], (LEN, DH), 1.0, 6.0, ((0, 16),))
    output = scatter_about(keys[3], (LEN, QH * DH), 0.25, 1.5, ((0, 16), (1, 2)))
    grad_output = scatter_about(keys[4], (LEN, QH * DH), 24.0, 144.0, ((0, 16), (1, 2)))
    log_norm = draw_log_norm(jax.random.fold_in(keys[7], 71), 0)
    stripe = jax.random.permutation(keys[6], N_SEQ).astype(jnp.int32)
    return {"query": query, "key_rows": key_rows, "value_rows": value_rows, "output": output, "grad_output": grad_output, "log_norm": log_norm, "stripe": stripe}


def block_terms(query_heads, grad_heads, lse_rows, delta_rows, key_block, value_block, diag_open):
    extent = key_block.shape[0]
    factor = key_block.shape[1] ** -0.5
    scores = jnp.einsum("shd,td->hst", query_heads, key_block) * factor
    row_ids = lax.broadcasted_iota(jnp.int32, (extent, extent), 0)
    col_ids = lax.broadcasted_iota(jnp.int32, (extent, extent), 1)
    allowed = (col_ids < row_ids) | ((col_ids == row_ids) & diag_open)
    weights = jnp.where(allowed[None], jnp.exp(scores - lse_rows[:, :, None]), jnp.float32(0.0))
    weights_low = lax.optimization_barrier(weights.astype(jnp.bfloat16)).astype(jnp.float32)
    grad_values = jnp.einsum("hst,shd->td", weights_low, grad_heads)
    grad_weights = jnp.einsum("shd,td->hst", grad_heads, value_block)
    grad_scores = (factor * weights * (grad_weights - delta_rows[:, :, None])).astype(jnp.bfloat16)
    grad_scores = lax.optimization_barrier(grad_scores).astype(jnp.float32)
    grad_query = jnp.einsum("hst,td->shd", grad_scores, key_block)
    grad_keys = jnp.einsum("hst,shd->td", grad_scores, query_heads)
    return grad_query, jnp.stack([grad_keys, grad_values])


def reference(query, key_rows, value_rows, output, grad_output, log_norm, stripe):
    query_blocks = query.reshape(N_SEQ, S_DEV, QH, DH)
    grad_blocks = grad_output.reshape(N_SEQ, S_DEV, QH, DH)
    output_blocks = output.reshape(N_SEQ, S_DEV, QH, DH)
    lse_blocks = log_norm.reshape(QH, N_SEQ, S_DEV).transpose(1, 0, 2)
    key_blocks = key_rows.reshape(N_SEQ, S_DEV, DH)
    value_blocks = value_rows.reshape(N_SEQ, S_DEV, DH)

    def one_block(grad_kv, block_index):
        query_heads = query_blocks[block_index].astype(jnp.float32)
        grad_heads = grad_blocks[block_index].astype(jnp.float32)
        delta_rows = jnp.sum(grad_heads * output_blocks[block_index].astype(jnp.float32), axis=2).T
        lse_rows = lse_blocks[block_index]
        grad_query = jnp.zeros((S_DEV, QH, DH), jnp.float32)
        for offset in range(WINDOW):
            source = ((block_index - offset) % N_SEQ).astype(jnp.int32)
            diag_open = stripe[source] <= stripe[block_index]
            key_block = key_blocks[source].astype(jnp.float32)
            value_block = value_blocks[source].astype(jnp.float32)
            query_part, kv_part = block_terms(query_heads, grad_heads, lse_rows, delta_rows, key_block, value_block, diag_open)
            grad_query = grad_query + query_part
            grad_kv = grad_kv.at[source].add(kv_part)
        return grad_kv, grad_query.astype(jnp.bfloat16)

    start_kv = jnp.zeros((N_SEQ, 2, S_DEV, DH), jnp.float32)
    grad_kv, grad_query = lax.scan(one_block, start_kv, jnp.arange(N_SEQ, dtype=jnp.int32))
    grad_key = grad_kv[:, 0].reshape(LEN, DH).astype(jnp.bfloat16)
    grad_value = grad_kv[:, 1].reshape(LEN, DH).astype(jnp.bfloat16)
    return grad_query.reshape(LEN, QH * DH), grad_key, grad_value
```

```python
import functools

import jax
import jax.numpy as jnp
from jax import lax
from jax.experimental import pallas as pl
from jax.experimental.pallas import tpu as pltpu
from jax.sharding import PartitionSpec as P

WINDOW = 8
GROUP = WINDOW // 2
LOG2E = 1.4426950408889634
F32 = jnp.float32
BF16 = jnp.bfloat16
OWN, NEAR, SIDE, FAR, MATE = range(5)
PAIRS = 3
QUADS = ((1, 1), (1, 0), (0, 0))
LAG = 3


def dot(a, b, ca, cb):
    return lax.dot_general(a, b, (((ca,), (cb,)), ((), ())), preferred_element_type=F32)


def kernel(
    n, stripe, q_hbm, k_hbm, v_hbm, o_hbm, g_hbm, lse_hbm,
    dq_out, dk_out, dv_out,
    q, g, o, lse, delta, level, qt, gt, kv, dqt, acc, take, part, rx, zs, fin, dq,
    in_sem, out_sem, kv_send, kv_recv, d_send, d_recv, p_send, p_recv, z_send, z_recv,
):
    me = lax.axis_index("seq")
    y = lax.axis_index("head")
    j = lax.rem(me, GROUP)
    base = me - j
    S, D2 = kv.shape[1:]
    D = D2 // 2
    H = q.shape[1] // D
    half = S // 2
    c = j % 2
    x = j // 2
    factor = D ** -0.5

    def mate(t):
        low = j % 2
        high = j // 2
        low = (1 - low) if t & 1 else low
        high = (1 - high) if t & 2 else high
        return high * 2 + low

    def at(t):
        return base + mate(t)

    def plane(d):
        return lax.rem(me + d * GROUP + n, n)

    loads = [
        pltpu.make_async_copy(k_hbm, kv.at[j, :, pl.ds(0, D)], in_sem.at[0]),
        pltpu.make_async_copy(v_hbm, kv.at[j, :, pl.ds(D, D)], in_sem.at[1]),
        pltpu.make_async_copy(q_hbm, q, in_sem.at[2]),
        pltpu.make_async_copy(g_hbm, g, in_sem.at[3]),
        pltpu.make_async_copy(o_hbm, o, in_sem.at[4]),
        pltpu.make_async_copy(lse_hbm, lse, in_sem.at[5]),
    ]
    for load in loads:
        load.start()

    def owner(t):
        i = mate(t)
        return lax.rem(base + i - jnp.where(i > j, 2 * GROUP, 0) + n, n)

    def partner(t):
        i = mate(t)
        return lax.rem(base + i + jnp.where(i > j, -2 * GROUP, 2 * GROUP) + n, n)

    barrier = pltpu.get_barrier_semaphore()
    peers = [(at(t), y) for t in (1, 2)] + [(at(t), 1 - y) for t in (0, 1, 2)]
    peers += [(plane(d), y) for d in (1, -1)]
    peers += [(partner(t), y) for t in (1, 2)]
    for p in peers:
        pl.semaphore_signal(barrier, inc=1, device_id=p, device_id_type=pl.DeviceIdType.MESH)
    for load in loads:
        load.wait()

    for h in range(H):
        cols = slice(h * D, (h + 1) * D)
        prod = g[:, cols].astype(F32) * o[:, cols].astype(F32)
        total = jnp.sum(prod, axis=1, keepdims=True) * factor
        delta[h] = jnp.broadcast_to(total, (S, D))
        line = jnp.broadcast_to(lse[h:h + 1, :] * LOG2E, (D, S))
        level[h] = line.T
        qt[h] = q[:, cols].T
        gt[h] = g[:, cols].T
    pl.semaphore_wait(barrier, len(peers))

    A = lambda i: i
    B = lambda i: GROUP + i
    C = 2 * GROUP

    def remote(src, dst, ss, rs, to):
        return pltpu.make_async_remote_copy(
            src_ref=src, dst_ref=dst, send_sem=ss, recv_sem=rs,
            device_id=to, device_id_type=pl.DeviceIdType.MESH,
        )

    def kv_copy(src, dst, sem, to):
        return remote(kv.at[src], kv.at[dst], kv_send.at[sem], kv_recv.at[dst], (to, y))

    up_b = kv_copy(A(j), B(j), 0, plane(1))
    up_c = kv_copy(B(j), C, 1, plane(1))
    own = {t: kv_copy(A(j), A(j), 1 + t, at(t)) for t in (1, 2)}
    late = {t: kv_copy(C, A(j), 1 + t, at(t)) for t in (1, 2)}
    b_out = {t: kv_copy(B(j), B(j), 3 + t, at(t)) for t in (1, 2)}
    b_relay = kv_copy(B(mate(2)), B(mate(2)), 6, at(1))
    a_relay = kv_copy(A(mate(2)), A(mate(2)), 7, at(1))

    def kv_arrived(slot):
        kv_copy(slot, slot, 0, at(1)).wait_recv()

    def on(core, *acts):
        @pl.when(c == core)
        def _():
            for act in acts:
                act()

    def spread_b():
        kv_arrived(B(j))
        b_out[1].start()
        b_out[2].start()
        pl.when(j > 0)(up_c.start)

    def relay_b():
        kv_arrived(B(mate(2)))
        b_relay.start()

    def relay_a():
        kv_arrived(A(mate(2)))
        a_relay.start()

    def pass_c():
        @pl.when(j > 0)
        def _():
            kv_arrived(C)
            pl.when(x == 1)(late[2].start)
            pl.when(c == 1)(late[1].start)

    def side_own():
        pl.when(x == 0)(own[2].start)

    on(1, up_b.start)
    on(0, own[1].start, side_own)

    dqt[...] = jnp.zeros_like(dqt)
    own_stripe = stripe[me]

    cols_ = lax.broadcasted_iota(jnp.int32, (half, half), 1)
    diff = lax.broadcasted_iota(jnp.int32, (half, half), 0) - cols_

    def rows(i):
        return slice(i * half, (i + 1) * half)

    def wide(a):
        return jnp.concatenate([a] * (half // D), axis=1)

    def pair(slot, least, k, h0):
        units = [(h, r, w) for h in (h0, h0 + 1) for r, w in QUADS]
        open_ = diff >= least
        ks = [kv[slot, rows(w), :D] for w in range(2)]
        vs = [kv[slot, rows(w), D:] for w in range(2)]
        dk, dv, dq_part = {}, {}, {}

        def products(unit):
            h, r, w = unit
            cols = slice(h * D, (h + 1) * D)
            return dot(q[rows(r), cols], ks[w], 1, 1), dot(g[rows(r), cols], vs[w], 1, 1)

        def add(sums, key, term):
            sums[key] = sums[key] + term if key in sums else term

        def use(unit, score, weight):
            h, r, w = unit
            p = jnp.exp2(score * (factor * LOG2E) - wide(level[h, rows(r)]))
            if r == w:
                p = jnp.where(open_, p, 0.0)
            d = (p * (weight * factor - wide(delta[h, rows(r)]))).astype(BF16)
            add(dv, w, dot(gt[h, :, rows(r)], p.astype(BF16), 1, 0))
            add(dk, w, dot(qt[h, :, rows(r)], d, 1, 0))
            add(dq_part, (h, r), dot(d, ks[w], 1, 0))
            if w == 0:
                dqt[h, rows(r)] += dq_part[h, r]

        waiting = []
        for unit in units:
            waiting.append((unit, products(unit)))
            if len(waiting) > LAG:
                unit, found = waiting.pop(0)
                use(unit, *found)
        for unit, found in waiting:
            use(unit, *found)
        for w in range(2):
            for m, total in enumerate((dk[w], dv[w])):
                if h0:
                    total = total + acc[k, w, m * D:(m + 1) * D, :]
                acc[k, w, m * D:(m + 1) * D, :] = total

    def compute(slot, late_flag, i, k, between):
        if late_flag:
            source = base - GROUP + i
        else:
            source = base + i - jnp.where(i > j, 2 * GROUP, 0)
        source = lax.rem(source + n, n)
        least = jnp.where(stripe[source] <= own_stripe, 0, 1)
        for h0 in range(0, H, 2):
            pair(slot, least, k, h0)
            if h0 == 0:
                between()

    def part_copies(kind):
        res = []
        if kind == SIDE:
            res.append(remote(part.at[kind, y], rx.at[kind, 0],
                              p_send.at[kind, 0], p_recv.at[kind, 0], (at(2), y)))
        to = at(2) if kind == SIDE else me
        res.append(remote(part.at[kind, 1 - y], rx.at[kind, 1],
                          p_send.at[kind, 1], p_recv.at[kind, 1], (to, 1 - y)))
        return res

    def send_part(kind):
        for copy in part_copies(kind):
            copy.start()

    def give(p):
        return remote(acc.at[2 * p + 1 + c], take.at[p], d_send.at[p], d_recv.at[p], (at(1), y))

    def join(p):
        give(p).wait_recv()
        part[NEAR + p] = (acc[2 * p + 2 - c] + take[p]).astype(BF16)
        send_part(NEAR + p)

    z_copies = [
        remote(zs.at[m], fin.at[m], z_send.at[m], z_recv.at[m], (to, y))
        for m, to in enumerate((plane(-1), owner(2), owner(1)))
    ]

    def forward(m, *kinds):
        total = arrived_part(kinds[0])
        for kind in kinds[1:]:
            total = total + arrived_part(kind)
        zs[m] = total.astype(BF16)
        z_copies[m].start()

    def arrived_part(kind):
        def get(m):
            remote(rx.at[kind, m], rx.at[kind, m], p_send.at[0, 0], p_recv.at[kind, m],
                   (at(1), y)).wait_recv()
            return rx[kind, m].astype(F32)

        first = part[kind, y].astype(F32) if kind != SIDE else get(0)
        return first + get(1)

    i_odd, i_even = 2 * x + 1, 2 * x
    o_odd, o_even = 3 - 2 * x, 2 - 2 * x

    def step0():
        on(0, up_b.start)
        on(1, side_own)

    compute(A(j), 0, j, 0, step0)
    part[OWN] = acc[0].astype(BF16)

    on(1, spread_b)
    on(0, lambda: kv_arrived(B(mate(1))))

    def step1():
        send_part(OWN)
        on(0, spread_b)

    compute(B(i_odd), 1, i_odd, 1, step1)
    on(0, give(0).start)
    on(1, lambda: kv_arrived(B(mate(1))))

    def step2():
        on(1, relay_b, lambda: join(0), pass_c)

    compute(B(i_even), 1, i_even, 2, step2)
    on(1, give(0).start)
    on(0, lambda: kv_arrived(B(mate(3))))

    def step3():
        on(0, relay_b, lambda: join(0), pass_c)

    compute(B(o_odd), 1, o_odd, 3, step3)
    on(0, give(1).start)
    on(1, lambda: kv_arrived(B(mate(3))))

    def step4():
        on(1, lambda: join(1), relay_a)

    compute(B(o_even), 1, o_even, 4, step4)
    on(1, give(1).start)
    on(0, lambda: kv_arrived(A(mate(3))))

    def step5():
        on(0, lambda: join(1))

    compute(A(o_odd), 0, o_odd, 5, step5)
    on(0, give(2).start)
    kv_arrived(A(mate(1)))

    def step6():
        on(1, lambda: join(2))
        on(0, relay_a)

    compute(A(mate(1)), 0, mate(1), 7, step6)
    part[MATE] = acc[7].astype(BF16)
    send_part(MATE)
    on(1, lambda: kv_arrived(A(mate(3))))

    def step7():
        pass

    compute(A(o_even), 0, o_even, 6, step7)
    on(1, give(2).start)
    forward(0, NEAR, SIDE)
    on(1, lambda: forward(1, FAR))
    on(0, lambda: join(2))
    forward(2, MATE)

    for h in range(H):
        dq[:, h * D:(h + 1) * D] = dqt[h].astype(BF16)
    dq_copy = pltpu.make_async_copy(dq, dq_out, out_sem)
    dq_copy.start()
    on(0, lambda: forward(1, FAR))

    mine = arrived_part(OWN)
    for copy, m in zip(z_copies, range(3)):
        copy.wait_recv()
        mine = mine + fin[m].astype(F32)
    dk_out[...] = mine[:D].T.astype(BF16)
    dv_out[...] = mine[D:].T.astype(BF16)

    for copy in [up_b, own[1], own[2], b_out[1], b_out[2], b_relay, a_relay]:
        copy.wait_send()
    pl.when(j > 0)(up_c.wait_send)
    for kind in range(5):
        for copy in part_copies(kind):
            copy.wait_send()
    for p in range(PAIRS):
        give(p).wait_send()
    for copy in z_copies:
        copy.wait_send()
    dq_copy.wait()


def shards(n, query, key_rows, value_rows, output, grad_output, log_norm, stripe):
    S, W = query.shape
    D = key_rows.shape[1]
    H = W // D
    half = S // 2
    any_ = pl.BlockSpec(memory_space=pl.ANY)
    vm = pl.BlockSpec(memory_space=pltpu.VMEM)
    dma = pltpu.SemaphoreType.DMA
    return pl.pallas_call(
        functools.partial(kernel, n),
        out_shape=(
            jax.ShapeDtypeStruct((S, W), BF16),
            jax.ShapeDtypeStruct((half, D), BF16),
            jax.ShapeDtypeStruct((half, D), BF16),
        ),
        in_specs=[pl.BlockSpec(memory_space=pltpu.SMEM)] + [any_] * 6,
        out_specs=(any_, vm, vm),
        scratch_shapes=[
            pltpu.VMEM((S, W), BF16),
            pltpu.VMEM((S, W), BF16),
            pltpu.VMEM((S, W), BF16),
            pltpu.VMEM((H, S), F32),
            pltpu.VMEM((H, S, D), F32),
            pltpu.VMEM((H, S, D), F32),
            pltpu.VMEM((H, D, S), BF16),
            pltpu.VMEM((H, D, S), BF16),
            pltpu.VMEM((2 * GROUP + 1, S, 2 * D), BF16),
            pltpu.VMEM((H, S, D), F32),
            pltpu.VMEM((WINDOW, 2, 2 * D, half), F32),
            pltpu.VMEM((PAIRS, 2, 2 * D, half), F32),
            pltpu.VMEM((5, 2, 2 * D, half), BF16),
            pltpu.VMEM((5, 2, 2 * D, half), BF16),
            pltpu.VMEM((3, 2 * D, half), BF16),
            pltpu.VMEM((3, 2 * D, half), BF16),
            pltpu.VMEM((S, W), BF16),
            dma((6,)),
            dma(()),
            dma((8,)),
            dma((2 * GROUP + 1,)),
            dma((PAIRS,)),
            dma((PAIRS,)),
            dma((5, 2)),
            dma((5, 2)),
            dma((3,)),
            dma((3,)),
        ],
        compiler_params=pltpu.CompilerParams(
            collective_id=0, has_side_effects=True, vmem_limit_bytes=67043328
        ),
        name="window_backward",
    )(stripe, query, key_rows, value_rows, output, grad_output, log_norm)


def solution(mesh):
    placed = (
        P("seq", "head"),
        P("seq", None),
        P("seq", None),
        P("seq", "head"),
        P("seq", "head"),
        P("head", "seq"),
        P(),
    )
    return jax.shard_map(
        functools.partial(shards, mesh.shape["seq"]),
        mesh=mesh,
        in_specs=placed,
        out_specs=(P("seq", "head"), P(("seq", "head"), None), P(("seq", "head"), None)),
        check_vma=False,
    )
```

```python
import functools

import jax
import jax.numpy as jnp
from jax import lax
from jax.experimental import pallas as pl
from jax.experimental.pallas import tpu as pltpu
from jax.sharding import PartitionSpec as P

WINDOW = 8
GROUP = WINDOW // 2
LOG2E = 1.4426950408889634
F32 = jnp.float32
BF16 = jnp.bfloat16
OWN, NEAR, SIDE, FAR, MATE = range(5)
PAIRS = 3
QUADS = ((1, 1), (1, 0), (0, 0))
LAG = 3


def dot(a, b, ca, cb):
    return lax.dot_general(a, b, (((ca,), (cb,)), ((), ())), preferred_element_type=F32)


def kernel(
    n, stripe_hbm, q_hbm, k_hbm, v_hbm, o_hbm, g_hbm, lse_hbm,
    dq_out, dk_out, dv_out,
    stripe, q, g, o, lse, delta, level, qt, gt, kv, dqt, acc, lend, take, part, rx, zs, fin,
    in_sem, kv_send, kv_recv, d_send, d_recv, p_send, p_recv, z_send, z_recv,
):
    me = lax.axis_index("seq")
    y = lax.axis_index("head")
    j = lax.rem(me, GROUP)
    base = me - j
    S, D2 = kv.shape[1:]
    D = D2 // 2
    H = q.shape[1] // D
    half = S // 2
    c = j % 2
    x = j // 2
    factor = D ** -0.5

    def mate(t):
        low = j % 2
        high = j // 2
        low = (1 - low) if t & 1 else low
        high = (1 - high) if t & 2 else high
        return high * 2 + low

    def at(t):
        return base + mate(t)

    def plane(d):
        return lax.rem(me + d * GROUP + n, n)

    loads = [
        pltpu.make_async_copy(k_hbm, kv.at[j, :, pl.ds(0, D)], in_sem.at[0]),
        pltpu.make_async_copy(v_hbm, kv.at[j, :, pl.ds(D, D)], in_sem.at[1]),
        pltpu.make_async_copy(q_hbm, q, in_sem.at[2]),
        pltpu.make_async_copy(g_hbm, g, in_sem.at[3]),
        pltpu.make_async_copy(o_hbm, o, in_sem.at[4]),
        pltpu.make_async_copy(lse_hbm, lse, in_sem.at[5]),
        pltpu.make_async_copy(stripe_hbm, stripe, in_sem.at[6]),
    ]
    for load in loads:
        load.start()

    def owner(t):
        i = mate(t)
        return lax.rem(base + i - jnp.where(i > j, 2 * GROUP, 0) + n, n)

    def partner(t):
        i = mate(t)
        return lax.rem(base + i + jnp.where(i > j, -2 * GROUP, 2 * GROUP) + n, n)

    barrier = pltpu.get_barrier_semaphore()
    peers = [(at(t), y) for t in (1, 2)] + [(at(t), 1 - y) for t in (0, 1, 2)]
    peers += [(plane(d), y) for d in (1, -1)]
    peers += [(partner(t), y) for t in (1, 2)]
    for p in peers:
        pl.semaphore_signal(barrier, inc=1, device_id=p, device_id_type=pl.DeviceIdType.MESH)
    loads[0].wait()
    loads[1].wait()
    pl.semaphore_wait(barrier, len(peers))

    A = lambda i: i
    B = lambda i: GROUP + i
    C = 2 * GROUP

    def remote(src, dst, ss, rs, to):
        return pltpu.make_async_remote_copy(
            src_ref=src, dst_ref=dst, send_sem=ss, recv_sem=rs,
            device_id=to, device_id_type=pl.DeviceIdType.MESH,
        )

    def kv_copy(src, dst, sem, to):
        return remote(kv.at[src], kv.at[dst], kv_send.at[sem], kv_recv.at[dst], (to, y))

    up_b = kv_copy(A(j), B(j), 0, plane(1))
    up_c = kv_copy(B(j), C, 1, plane(1))
    own = {t: kv_copy(A(j), A(j), 1 + t, at(t)) for t in (1, 2)}
    late = {t: kv_copy(C, A(j), 1 + t, at(t)) for t in (1, 2)}
    b_out = {t: kv_copy(B(j), B(j), 3 + t, at(t)) for t in (1, 2)}
    b_relay = kv_copy(B(mate(2)), B(mate(2)), 6, at(1))
    a_relay = kv_copy(A(mate(2)), A(mate(2)), 7, at(1))

    def kv_arrived(slot):
        kv_copy(slot, slot, 0, at(1)).wait_recv()

    def on(core, *acts):
        @pl.when(c == core)
        def _():
            for act in acts:
                act()

    def spread_b():
        kv_arrived(B(j))
        b_out[1].start()
        b_out[2].start()
        pl.when(j > 0)(up_c.start)

    def relay_b():
        kv_arrived(B(mate(2)))
        b_relay.start()

    def relay_a():
        kv_arrived(A(mate(2)))
        a_relay.start()

    def pass_c():
        @pl.when(j > 0)
        def _():
            kv_arrived(C)
            pl.when(x == 1)(late[2].start)
            pl.when(c == 1)(late[1].start)

    def side_own():
        pl.when(x == 0)(own[2].start)

    on(1, up_b.start)
    on(0, own[1].start, side_own)

    for load in loads[2:]:
        load.wait()

    for h in range(H):
        cols = slice(h * D, (h + 1) * D)
        prod = g[:, cols].astype(F32) * o[:, cols].astype(F32)
        total = jnp.sum(prod, axis=1, keepdims=True) * factor
        delta[h] = jnp.broadcast_to(total, (S, D))
        line = jnp.broadcast_to(lse[h:h + 1, :] * LOG2E, (D, S))
        level[h] = line.T
        qt[h] = q[:, cols].T
        gt[h] = g[:, cols].T
    dqt[...] = jnp.zeros_like(dqt)
    own_stripe = stripe[me]

    cols_ = lax.broadcasted_iota(jnp.int32, (half, half), 1)
    diff = lax.broadcasted_iota(jnp.int32, (half, half), 0) - cols_

    def rows(i):
        return slice(i * half, (i + 1) * half)

    def wide(a):
        return jnp.concatenate([a] * (half // D), axis=1)

    def pair(slot, least, k, h0):
        units = [(h, r, w) for h in (h0, h0 + 1) for r, w in QUADS]
        open_ = diff >= least
        ks = [kv[slot, rows(w), :D] for w in range(2)]
        vs = [kv[slot, rows(w), D:] for w in range(2)]
        dk, dv, dq_part = {}, {}, {}

        def products(unit):
            h, r, w = unit
            cols = slice(h * D, (h + 1) * D)
            return dot(q[rows(r), cols], ks[w], 1, 1), dot(g[rows(r), cols], vs[w], 1, 1)

        def add(sums, key, term):
            sums[key] = sums[key] + term if key in sums else term

        def use(unit, score, weight):
            h, r, w = unit
            p = jnp.exp2(score * (factor * LOG2E) - wide(level[h, rows(r)]))
            if r == w:
                p = jnp.where(open_, p, 0.0)
            d = (p * (weight * factor - wide(delta[h, rows(r)]))).astype(BF16)
            add(dv, w, dot(gt[h, :, rows(r)], p.astype(BF16), 1, 0))
            add(dk, w, dot(qt[h, :, rows(r)], d, 1, 0))
            add(dq_part, (h, r), dot(d, ks[w], 1, 0))
            if w == 0:
                dqt[h, rows(r)] += dq_part[h, r]

        waiting = []
        for unit in units:
            waiting.append((unit, products(unit)))
            if len(waiting) > LAG:
                unit, found = waiting.pop(0)
                use(unit, *found)
        for unit, found in waiting:
            use(unit, *found)
        for w in range(2):
            for m, total in enumerate((dk[w], dv[w])):
                if h0:
                    total = total + acc[k, w, m * D:(m + 1) * D, :]
                acc[k, w, m * D:(m + 1) * D, :] = total

    def compute(slot, late_flag, i, k, between):
        if late_flag:
            source = base - GROUP + i
        else:
            source = base + i - jnp.where(i > j, 2 * GROUP, 0)
        source = lax.rem(source + n, n)
        least = jnp.where(stripe[source] <= own_stripe, 0, 1)
        for h0 in range(0, H, 2):
            pair(slot, least, k, h0)
            if h0 == 0:
                between()

    def part_copies(kind):
        res = []
        if kind == SIDE:
            res.append(remote(part.at[kind, y], rx.at[kind, 0],
                              p_send.at[kind, 0], p_recv.at[kind, 0], (at(2), y)))
        to = at(2) if kind == SIDE else me
        res.append(remote(part.at[kind, 1 - y], rx.at[kind, 1],
                          p_send.at[kind, 1], p_recv.at[kind, 1], (to, 1 - y)))
        return res

    def send_part(kind):
        for copy in part_copies(kind):
            copy.start()

    def give(p):
        return remote(lend.at[p], take.at[p], d_send.at[p], d_recv.at[p], (at(1), y))

    def lend_out(p):
        lend[p] = acc[2 * p + 1 + c].astype(BF16)
        give(p).start()

    def join(p):
        give(p).wait_recv()
        part[NEAR + p] = (acc[2 * p + 2 - c] + take[p].astype(F32)).astype(BF16)
        send_part(NEAR + p)

    z_copies = [
        remote(zs.at[m], fin.at[m], z_send.at[m], z_recv.at[m], (to, y))
        for m, to in enumerate((plane(-1), owner(2), owner(1)))
    ]

    def forward(m, *kinds):
        total = arrived_part(kinds[0])
        for kind in kinds[1:]:
            total = total + arrived_part(kind)
        zs[m] = total.astype(BF16)
        z_copies[m].start()

    def arrived_part(kind):
        def get(m):
            remote(rx.at[kind, m], rx.at[kind, m], p_send.at[0, 0], p_recv.at[kind, m],
                   (at(1), y)).wait_recv()
            return rx[kind, m].astype(F32)

        first = part[kind, y].astype(F32) if kind != SIDE else get(0)
        return first + get(1)

    i_odd, i_even = 2 * x + 1, 2 * x
    o_odd, o_even = 3 - 2 * x, 2 - 2 * x

    on(0, up_b.start)
    on(1, side_own)

    compute(A(j), 0, j, 0, lambda: None)
    part[OWN] = acc[0].astype(BF16)
    on(1, spread_b)
    on(0, lambda: kv_arrived(B(mate(1))))

    def step1():
        send_part(OWN)
        on(0, spread_b)

    compute(B(i_odd), 1, i_odd, 1, step1)
    on(0, lambda: lend_out(0))
    on(1, lambda: kv_arrived(B(mate(1))))

    def step2():
        on(1, relay_b, lambda: join(0), pass_c)

    compute(B(i_even), 1, i_even, 2, step2)
    on(1, lambda: lend_out(0))
    kv_arrived(A(mate(1)))

    def step3():
        on(0, relay_b, lambda: join(0), pass_c)

    compute(A(mate(1)), 0, mate(1), 7, step3)
    part[MATE] = acc[7].astype(BF16)
    on(0, lambda: kv_arrived(B(mate(3))))

    def step4():
        send_part(MATE)
        on(1, relay_a)

    compute(B(o_odd), 1, o_odd, 3, step4)
    on(0, lambda: lend_out(1))
    on(1, lambda: kv_arrived(B(mate(3))))

    def step5():
        on(1, lambda: join(1))
        on(0, relay_a)

    compute(B(o_even), 1, o_even, 4, step5)
    on(1, lambda: lend_out(1))
    on(0, lambda: kv_arrived(A(mate(3))))

    def step6():
        on(0, lambda: join(1))
        forward(2, MATE)

    compute(A(o_odd), 0, o_odd, 5, step6)
    on(0, lambda: lend_out(2))
    on(1, lambda: kv_arrived(A(mate(3))))

    def step7():
        on(1, lambda: join(2))

    compute(A(o_even), 0, o_even, 6, step7)
    on(1, lambda: lend_out(2))

    for h in range(H):
        dq_out[:, h * D:(h + 1) * D] = dqt[h].astype(BF16)
    on(0, lambda: join(2))
    forward(0, NEAR, SIDE)
    forward(1, FAR)

    mine = arrived_part(OWN)
    for copy, m in zip(z_copies, range(3)):
        copy.wait_recv()
        mine = mine + fin[m].astype(F32)
    dk_out[...] = mine[:D].T.astype(BF16)
    dv_out[...] = mine[D:].T.astype(BF16)

    for copy in [up_b, own[1], own[2], b_out[1], b_out[2], b_relay, a_relay]:
        copy.wait_send()
    pl.when(j > 0)(up_c.wait_send)
    for kind in range(5):
        for copy in part_copies(kind):
            copy.wait_send()
    for p in range(PAIRS):
        give(p).wait_send()
    for copy in z_copies:
        copy.wait_send()


def emit(*refs):
    copies = [pltpu.make_async_copy(refs[m], refs[3 + m], refs[6].at[m]) for m in range(3)]
    for copy in copies:
        copy.start()
    for copy in copies:
        copy.wait()


def shards(n, query, key_rows, value_rows, output, grad_output, log_norm, stripe):
    S, W = query.shape
    D = key_rows.shape[1]
    H = W // D
    half = S // 2
    any_ = pl.BlockSpec(memory_space=pl.ANY)
    vm = pl.BlockSpec(memory_space=pltpu.VMEM)
    dma = pltpu.SemaphoreType.DMA
    arrays = (stripe, query, key_rows, value_rows, output, grad_output, log_norm)
    found = pl.pallas_call(
        functools.partial(kernel, n),
        out_shape=(
            jax.ShapeDtypeStruct((S, W), BF16),
            jax.ShapeDtypeStruct((half, D), BF16),
            jax.ShapeDtypeStruct((half, D), BF16),
        ),
        in_specs=[pl.BlockSpec(memory_space=pltpu.HBM)] * 7,
        out_specs=(vm, vm, vm),
        scratch_shapes=[
            pltpu.SMEM(stripe.shape, jnp.int32),
            pltpu.VMEM((S, W), BF16),
            pltpu.VMEM((S, W), BF16),
            pltpu.VMEM((S, W), BF16),
            pltpu.VMEM((H, S), F32),
            pltpu.VMEM((H, S, D), F32),
            pltpu.VMEM((H, S, D), F32),
            pltpu.VMEM((H, D, S), BF16),
            pltpu.VMEM((H, D, S), BF16),
            pltpu.VMEM((2 * GROUP + 1, S, 2 * D), BF16),
            pltpu.VMEM((H, S, D), F32),
            pltpu.VMEM((WINDOW, 2, 2 * D, half), F32),
            pltpu.VMEM((PAIRS, 2, 2 * D, half), BF16),
            pltpu.VMEM((PAIRS, 2, 2 * D, half), BF16),
            pltpu.VMEM((5, 2, 2 * D, half), BF16),
            pltpu.VMEM((5, 2, 2 * D, half), BF16),
            pltpu.VMEM((3, 2 * D, half), BF16),
            pltpu.VMEM((3, 2 * D, half), BF16),
            dma((7,)),
            dma((8,)),
            dma((2 * GROUP + 1,)),
            dma((PAIRS,)),
            dma((PAIRS,)),
            dma((5, 2)),
            dma((5, 2)),
            dma((3,)),
            dma((3,)),
        ],
        compiler_params=pltpu.CompilerParams(
            collective_id=0, has_side_effects=True, vmem_limit_bytes=33554432
        ),
        name="window_backward",
    )(*(pltpu.with_memory_space_constraint(a, pltpu.HBM) for a in arrays))
    return pl.pallas_call(
        emit,
        out_shape=tuple(jax.ShapeDtypeStruct(a.shape, a.dtype) for a in found),
        in_specs=[vm] * 3,
        out_specs=(any_,) * 3,
        scratch_shapes=[dma((3,))],
        compiler_params=pltpu.CompilerParams(vmem_limit_bytes=1 << 22),
        name="emit",
    )(*found)


def solution(mesh):
    placed = (
        P("seq", "head"),
        P("seq", None),
        P("seq", None),
        P("seq", "head"),
        P("seq", "head"),
        P("head", "seq"),
        P(),
    )
    return jax.shard_map(
        functools.partial(shards, mesh.shape["seq"]),
        mesh=mesh,
        in_specs=placed,
        out_specs=(P("seq", "head"), P(("seq", "head"), None), P(("seq", "head"), None)),
        check_vma=False,
    )
```

```python
import functools

import jax
import jax.numpy as jnp
from jax import lax
from jax.experimental import pallas as pl
from jax.experimental.pallas import tpu as pltpu
from jax.sharding import PartitionSpec as P

WINDOW = 8
GROUP = WINDOW // 2
LOG2E = 1.4426950408889634
F32 = jnp.float32
BF16 = jnp.bfloat16
OWN, NEAR, SIDE, FAR, MATE = range(5)
PAIRS = 3
QUADS = ((1, 1), (1, 0), (0, 0))
LAG = 3


def dot(a, b, ca, cb):
    return lax.dot_general(a, b, (((ca,), (cb,)), ((), ())), preferred_element_type=F32)


def kernel(
    n, stripe_hbm, q_hbm, k_hbm, v_hbm, o_hbm, g_hbm, lse_hbm,
    dq_out, dk_out, dv_out,
    stripe, q, g, o, lse, delta, level, qt, gt, kv, dqt, acc, lend, take, part, rx, zs, fin,
    in_sem, kv_send, kv_recv, d_send, d_recv, p_send, p_recv, z_send, z_recv,
):
    me = lax.axis_index("seq")
    y = lax.axis_index("head")
    j = lax.rem(me, GROUP)
    base = me - j
    S, D2 = kv.shape[1:]
    D = D2 // 2
    H = q.shape[1] // D
    half = S // 2
    c = j % 2
    x = j // 2
    factor = D ** -0.5

    def mate(t):
        low = j % 2
        high = j // 2
        low = (1 - low) if t & 1 else low
        high = (1 - high) if t & 2 else high
        return high * 2 + low

    def at(t):
        return base + mate(t)

    def plane(d):
        return lax.rem(me + d * GROUP + n, n)

    loads = [
        pltpu.make_async_copy(k_hbm, kv.at[j, :, pl.ds(0, D)], in_sem.at[0]),
        pltpu.make_async_copy(v_hbm, kv.at[j, :, pl.ds(D, D)], in_sem.at[1]),
        pltpu.make_async_copy(q_hbm, q, in_sem.at[2]),
        pltpu.make_async_copy(g_hbm, g, in_sem.at[3]),
        pltpu.make_async_copy(o_hbm, o, in_sem.at[4]),
        pltpu.make_async_copy(lse_hbm, lse, in_sem.at[5]),
        pltpu.make_async_copy(stripe_hbm, stripe, in_sem.at[6]),
    ]
    for load in loads:
        load.start()

    def owner(t):
        i = mate(t)
        return lax.rem(base + i - jnp.where(i > j, 2 * GROUP, 0) + n, n)

    def partner(t):
        i = mate(t)
        return lax.rem(base + i + jnp.where(i > j, -2 * GROUP, 2 * GROUP) + n, n)

    barrier = pltpu.get_barrier_semaphore()
    peers = [(at(t), y) for t in (1, 2)] + [(at(t), 1 - y) for t in (0, 1, 2)]
    peers += [(plane(d), y) for d in (1, -1)]
    peers += [(partner(t), y) for t in (1, 2)]
    for p in peers:
        pl.semaphore_signal(barrier, inc=1, device_id=p, device_id_type=pl.DeviceIdType.MESH)
    loads[0].wait()
    loads[1].wait()
    pl.semaphore_wait(barrier, len(peers))

    A = lambda i: i
    B = lambda i: GROUP + i
    C = 2 * GROUP

    def remote(src, dst, ss, rs, to):
        return pltpu.make_async_remote_copy(
            src_ref=src, dst_ref=dst, send_sem=ss, recv_sem=rs,
            device_id=to, device_id_type=pl.DeviceIdType.MESH,
        )

    def kv_copy(src, dst, sem, to):
        return remote(kv.at[src], kv.at[dst], kv_send.at[sem], kv_recv.at[dst], (to, y))

    up_b = kv_copy(A(j), B(j), 0, plane(1))
    up_c = kv_copy(B(j), C, 1, plane(1))
    own = {t: kv_copy(A(j), A(j), 1 + t, at(t)) for t in (1, 2)}
    late = {t: kv_copy(C, A(j), 1 + t, at(t)) for t in (1, 2)}
    b_out = {t: kv_copy(B(j), B(j), 3 + t, at(t)) for t in (1, 2)}
    b_relay = kv_copy(B(mate(2)), B(mate(2)), 6, at(1))
    a_relay = kv_copy(A(mate(2)), A(mate(2)), 7, at(1))

    def kv_arrived(slot):
        kv_copy(slot, slot, 0, at(1)).wait_recv()

    def on(core, *acts):
        @pl.when(c == core)
        def _():
            for act in acts:
                act()

    def spread_b():
        kv_arrived(B(j))
        b_out[1].start()
        b_out[2].start()
        pl.when(j > 0)(up_c.start)

    def relay_b():
        kv_arrived(B(mate(2)))
        b_relay.start()

    def relay_a():
        kv_arrived(A(mate(2)))
        a_relay.start()

    def pass_c():
        @pl.when(j > 0)
        def _():
            kv_arrived(C)
            pl.when(x == 1)(late[2].start)
            pl.when(c == 1)(late[1].start)

    def side_own():
        pl.when(x == 0)(own[2].start)

    on(1, up_b.start)
    on(0, own[1].start, side_own)

    for load in loads[2:]:
        load.wait()

    for h in range(H):
        cols = slice(h * D, (h + 1) * D)
        prod = g[:, cols].astype(F32) * o[:, cols].astype(F32)
        total = jnp.sum(prod, axis=1, keepdims=True) * factor
        delta[h] = jnp.broadcast_to(total, (S, D))
        line = jnp.broadcast_to(lse[h:h + 1, :] * LOG2E, (D, S))
        level[h] = line.T
        qt[h] = q[:, cols].T
        gt[h] = g[:, cols].T
    dqt[...] = jnp.zeros_like(dqt)
    own_stripe = stripe[me]

    cols_ = lax.broadcasted_iota(jnp.int32, (half, half), 1)
    diff = lax.broadcasted_iota(jnp.int32, (half, half), 0) - cols_

    def rows(i):
        return slice(i * half, (i + 1) * half)

    def wide(a):
        return jnp.concatenate([a] * (half // D), axis=1)

    def pair(slot, least, k, h0):
        units = [(h, r, w) for h in (h0, h0 + 1) for r, w in QUADS]
        open_ = diff >= least
        ks = [kv[slot, rows(w), :D] for w in range(2)]
        vs = [kv[slot, rows(w), D:] for w in range(2)]
        dk, dv, dq_part = {}, {}, {}

        def products(unit):
            h, r, w = unit
            cols = slice(h * D, (h + 1) * D)
            return dot(q[rows(r), cols], ks[w], 1, 1), dot(g[rows(r), cols], vs[w], 1, 1)

        def add(sums, key, term):
            sums[key] = sums[key] + term if key in sums else term

        def use(unit, score, weight):
            h, r, w = unit
            p = jnp.exp2(score * (factor * LOG2E) - wide(level[h, rows(r)]))
            if r == w:
                p = jnp.where(open_, p, 0.0)
            d = (p * (weight * factor - wide(delta[h, rows(r)]))).astype(BF16)
            add(dv, w, dot(gt[h, :, rows(r)], p.astype(BF16), 1, 0))
            add(dk, w, dot(qt[h, :, rows(r)], d, 1, 0))
            add(dq_part, (h, r), dot(d, ks[w], 1, 0))
            if w == 0:
                dqt[h, rows(r)] += dq_part[h, r]

        waiting = []
        for unit in units:
            waiting.append((unit, products(unit)))
            if len(waiting) > LAG:
                unit, found = waiting.pop(0)
                use(unit, *found)
        for unit, found in waiting:
            use(unit, *found)
        for w in range(2):
            for m, total in enumerate((dk[w], dv[w])):
                if h0:
                    total = total + acc[k, w, m * D:(m + 1) * D, :]
                acc[k, w, m * D:(m + 1) * D, :] = total

    def near(i):
        return B(i), base - GROUP + i

    def side(i):
        return A(i), base + i - jnp.where(i > j, 2 * GROUP, 0)

    def compute(block, k, between):
        slot, source = block
        source = lax.rem(source + n, n)
        least = jnp.where(stripe[source] <= own_stripe, 0, 1)
        for h0 in range(0, H, 2):
            pair(slot, least, k, h0)
            if h0 == 0:
                between()

    def part_copies(kind):
        res = []
        if kind == SIDE:
            res.append(remote(part.at[kind, y], rx.at[kind, 0],
                              p_send.at[kind, 0], p_recv.at[kind, 0], (at(2), y)))
        to = at(2) if kind == SIDE else me
        res.append(remote(part.at[kind, 1 - y], rx.at[kind, 1],
                          p_send.at[kind, 1], p_recv.at[kind, 1], (to, 1 - y)))
        return res

    def send_part(kind):
        for copy in part_copies(kind):
            copy.start()

    def give(p):
        return remote(lend.at[p], take.at[p], d_send.at[p], d_recv.at[p], (at(1), y))

    def lend_out(p):
        lend[p] = acc[2 * p + 1 + c].astype(BF16)
        give(p).start()

    def join(p):
        give(p).wait_recv()
        part[NEAR + p] = (acc[2 * p + 2 - c] + take[p].astype(F32)).astype(BF16)
        send_part(NEAR + p)

    z_copies = [
        remote(zs.at[m], fin.at[m], z_send.at[m], z_recv.at[m], (to, y))
        for m, to in enumerate((plane(-1), owner(2), owner(1)))
    ]

    def forward(m, *kinds):
        total = arrived_part(kinds[0])
        for kind in kinds[1:]:
            total = total + arrived_part(kind)
        zs[m] = total.astype(BF16)
        z_copies[m].start()

    def arrived_part(kind):
        def get(m):
            remote(rx.at[kind, m], rx.at[kind, m], p_send.at[0, 0], p_recv.at[kind, m],
                   (at(1), y)).wait_recv()
            return rx[kind, m].astype(F32)

        first = part[kind, y].astype(F32) if kind != SIDE else get(0)
        return first + get(1)

    i_odd, i_even = 2 * x + 1, 2 * x
    o_odd, o_even = 3 - 2 * x, 2 - 2 * x

    on(0, up_b.start)
    on(1, side_own)

    def either(at0, at1):
        return (1 - c) * at0 + c * at1

    compute(side(j), 0, lambda: None)
    part[OWN] = acc[0].astype(BF16)
    on(1, spread_b, lambda: kv_arrived(A(mate(1))))
    on(0, lambda: kv_arrived(B(mate(1))))

    def step1():
        send_part(OWN)
        on(0, spread_b)

    compute(near(i_odd), 1, step1)
    on(0, lambda: lend_out(0))

    even, own_side = near(i_even), side(mate(1))
    compute(tuple(map(either, even, own_side)), either(2, 7), lambda: None)
    on(0, lambda: kv_arrived(A(mate(1))))
    on(1, pass_c, lambda: kv_arrived(B(mate(1))))

    def step3():
        on(0, pass_c)
        on(1, lambda: join(0))

    compute(tuple(map(either, own_side, even)), either(7, 2), step3)
    part[MATE] = acc[7].astype(BF16)
    on(0, lambda: kv_arrived(B(mate(3))))
    on(1, lambda: lend_out(0), relay_b)

    def step4():
        send_part(MATE)
        on(0, relay_b, lambda: join(0))

    compute(near(o_odd), 3, step4)
    on(0, lambda: lend_out(1))
    on(1, lambda: kv_arrived(B(mate(3))))

    def step5():
        on(1, relay_a, lambda: join(1))

    compute(near(o_even), 4, step5)
    on(1, lambda: lend_out(1))
    on(0, lambda: kv_arrived(A(mate(3))))

    def step6():
        on(0, relay_a, lambda: join(1))

    compute(side(o_odd), 5, step6)
    on(0, lambda: lend_out(2))
    on(1, lambda: kv_arrived(A(mate(3))))

    def step7():
        forward(2, MATE)

    compute(side(o_even), 6, step7)
    on(1, lambda: lend_out(2))

    for h in range(H):
        dq_out[:, h * D:(h + 1) * D] = dqt[h].astype(BF16)
    join(2)
    forward(0, NEAR, SIDE)
    forward(1, FAR)

    mine = arrived_part(OWN)
    for copy, m in zip(z_copies, range(3)):
        copy.wait_recv()
        mine = mine + fin[m].astype(F32)
    dk_out[...] = mine[:D].T.astype(BF16)
    dv_out[...] = mine[D:].T.astype(BF16)

    for copy in [up_b, own[1], own[2], b_out[1], b_out[2], b_relay, a_relay]:
        copy.wait_send()
    pl.when(j > 0)(up_c.wait_send)
    for kind in range(5):
        for copy in part_copies(kind):
            copy.wait_send()
    for p in range(PAIRS):
        give(p).wait_send()
    for copy in z_copies:
        copy.wait_send()


def emit(*refs):
    copies = [pltpu.make_async_copy(refs[m], refs[3 + m], refs[6].at[m]) for m in range(3)]
    for copy in copies:
        copy.start()
    for copy in copies:
        copy.wait()


def shards(n, query, key_rows, value_rows, output, grad_output, log_norm, stripe):
    S, W = query.shape
    D = key_rows.shape[1]
    H = W // D
    half = S // 2
    any_ = pl.BlockSpec(memory_space=pl.ANY)
    vm = pl.BlockSpec(memory_space=pltpu.VMEM)
    dma = pltpu.SemaphoreType.DMA
    arrays = (stripe, query, key_rows, value_rows, output, grad_output, log_norm)
    found = pl.pallas_call(
        functools.partial(kernel, n),
        out_shape=(
            jax.ShapeDtypeStruct((S, W), BF16),
            jax.ShapeDtypeStruct((half, D), BF16),
            jax.ShapeDtypeStruct((half, D), BF16),
        ),
        in_specs=[pl.BlockSpec(memory_space=pltpu.HBM)] * 7,
        out_specs=(vm, vm, vm),
        scratch_shapes=[
            pltpu.SMEM(stripe.shape, jnp.int32),
            pltpu.VMEM((S, W), BF16),
            pltpu.VMEM((S, W), BF16),
            pltpu.VMEM((S, W), BF16),
            pltpu.VMEM((H, S), F32),
            pltpu.VMEM((H, S, D), F32),
            pltpu.VMEM((H, S, D), F32),
            pltpu.VMEM((H, D, S), BF16),
            pltpu.VMEM((H, D, S), BF16),
            pltpu.VMEM((2 * GROUP + 1, S, 2 * D), BF16),
            pltpu.VMEM((H, S, D), F32),
            pltpu.VMEM((WINDOW, 2, 2 * D, half), F32),
            pltpu.VMEM((PAIRS, 2, 2 * D, half), BF16),
            pltpu.VMEM((PAIRS, 2, 2 * D, half), BF16),
            pltpu.VMEM((5, 2, 2 * D, half), BF16),
            pltpu.VMEM((5, 2, 2 * D, half), BF16),
            pltpu.VMEM((3, 2 * D, half), BF16),
            pltpu.VMEM((3, 2 * D, half), BF16),
            dma((7,)),
            dma((8,)),
            dma((2 * GROUP + 1,)),
            dma((PAIRS,)),
            dma((PAIRS,)),
            dma((5, 2)),
            dma((5, 2)),
            dma((3,)),
            dma((3,)),
        ],
        compiler_params=pltpu.CompilerParams(
            collective_id=0, has_side_effects=True, vmem_limit_bytes=33554432
        ),
        name="window_backward",
    )(*(pltpu.with_memory_space_constraint(a, pltpu.HBM) for a in arrays))
    return pl.pallas_call(
        emit,
        out_shape=tuple(jax.ShapeDtypeStruct(a.shape, a.dtype) for a in found),
        in_specs=[vm] * 3,
        out_specs=(any_,) * 3,
        scratch_shapes=[dma((3,))],
        compiler_params=pltpu.CompilerParams(vmem_limit_bytes=1 << 22),
        name="emit",
    )(*found)


def solution(mesh):
    placed = (
        P("seq", "head"),
        P("seq", None),
        P("seq", None),
        P("seq", "head"),
        P("seq", "head"),
        P("head", "seq"),
        P(),
    )
    return jax.shard_map(
        functools.partial(shards, mesh.shape["seq"]),
        mesh=mesh,
        in_specs=placed,
        out_specs=(P("seq", "head"), P(("seq", "head"), None), P(("seq", "head"), None)),
        check_vma=False,
    )
```

```python
import functools

import jax
import jax.numpy as jnp
from jax import lax
from jax.experimental import pallas as pl
from jax.experimental.pallas import tpu as pltpu
from jax.sharding import PartitionSpec as P

WINDOW = 8
GROUP = WINDOW // 2
LOG2E = 1.4426950408889634
F32 = jnp.float32
BF16 = jnp.bfloat16
OWN, NEAR, SIDE, FAR, MATE = range(5)
PAIRS = 3
QUADS = ((0, 0), (1, 0), (1, 1))
LAG = 3


def dot(a, b, ca, cb):
    return lax.dot_general(a, b, (((ca,), (cb,)), ((), ())), preferred_element_type=F32)


def kernel(
    n, stripe_hbm, q_hbm, k_hbm, v_hbm, o_hbm, g_hbm, lse_hbm,
    dq_out, dk_out, dv_out,
    stripe, q, g, o, lse, delta, level, qt, gt, kv, dqt, acc, lend, take, part, rx, zs, fin,
    in_sem, kv_send, kv_recv, d_send, d_recv, p_send, p_recv, z_send, z_recv,
):
    me = lax.axis_index("seq")
    y = lax.axis_index("head")
    j = lax.rem(me, GROUP)
    base = me - j
    S, D2 = kv.shape[1:]
    D = D2 // 2
    H = q.shape[1] // D
    half = S // 2
    c = j % 2
    x = j // 2
    factor = D ** -0.5

    def mate(t):
        low = j % 2
        high = j // 2
        low = (1 - low) if t & 1 else low
        high = (1 - high) if t & 2 else high
        return high * 2 + low

    def at(t):
        return base + mate(t)

    def plane(d):
        return lax.rem(me + d * GROUP + n, n)

    loads = [
        pltpu.make_async_copy(k_hbm, kv.at[j, :, pl.ds(0, D)], in_sem.at[0]),
        pltpu.make_async_copy(v_hbm, kv.at[j, :, pl.ds(D, D)], in_sem.at[1]),
        pltpu.make_async_copy(q_hbm, q, in_sem.at[2]),
        pltpu.make_async_copy(g_hbm, g, in_sem.at[3]),
        pltpu.make_async_copy(o_hbm, o, in_sem.at[4]),
        pltpu.make_async_copy(lse_hbm, lse, in_sem.at[5]),
        pltpu.make_async_copy(stripe_hbm, stripe, in_sem.at[6]),
    ]
    for load in loads:
        load.start()

    def owner(t):
        i = mate(t)
        return lax.rem(base + i - jnp.where(i > j, 2 * GROUP, 0) + n, n)

    def partner(t):
        i = mate(t)
        return lax.rem(base + i + jnp.where(i > j, -2 * GROUP, 2 * GROUP) + n, n)

    barrier = pltpu.get_barrier_semaphore()
    peers = [(at(t), y) for t in (1, 2)] + [(at(t), 1 - y) for t in (0, 1, 2)]
    peers += [(plane(d), y) for d in (1, -1)]
    peers += [(partner(t), y) for t in (1, 2)]
    for p in peers:
        pl.semaphore_signal(barrier, inc=1, device_id=p, device_id_type=pl.DeviceIdType.MESH)
    loads[0].wait()
    loads[1].wait()
    pl.semaphore_wait(barrier, len(peers))

    A = lambda i: i
    B = lambda i: GROUP + i
    C = 2 * GROUP

    def remote(src, dst, ss, rs, to):
        return pltpu.make_async_remote_copy(
            src_ref=src, dst_ref=dst, send_sem=ss, recv_sem=rs,
            device_id=to, device_id_type=pl.DeviceIdType.MESH,
        )

    def kv_copy(src, dst, sem, to):
        return remote(kv.at[src], kv.at[dst], kv_send.at[sem], kv_recv.at[dst], (to, y))

    up_b = kv_copy(A(j), B(j), 0, plane(1))
    up_c = kv_copy(B(j), C, 1, plane(1))
    own = {t: kv_copy(A(j), A(j), 1 + t, at(t)) for t in (1, 2)}
    late = {t: kv_copy(C, A(j), 1 + t, at(t)) for t in (1, 2)}
    b_out = {t: kv_copy(B(j), B(j), 3 + t, at(t)) for t in (1, 2)}
    b_relay = kv_copy(B(mate(2)), B(mate(2)), 6, at(1))
    a_relay = kv_copy(A(mate(2)), A(mate(2)), 7, at(1))

    def kv_arrived(slot):
        kv_copy(slot, slot, 0, at(1)).wait_recv()

    def on(core, *acts):
        @pl.when(c == core)
        def _():
            for act in acts:
                act()

    def spread_b():
        kv_arrived(B(j))
        b_out[1].start()
        b_out[2].start()
        pl.when(j > 0)(up_c.start)

    def relay_b():
        kv_arrived(B(mate(2)))
        b_relay.start()

    def relay_a():
        kv_arrived(A(mate(2)))
        a_relay.start()

    def pass_c():
        @pl.when(j > 0)
        def _():
            kv_arrived(C)
            pl.when(x == 1)(late[2].start)
            pl.when(c == 1)(late[1].start)

    def side_own():
        pl.when(x == 0)(own[2].start)

    on(1, up_b.start)
    on(0, own[1].start, side_own)

    for load in loads[2:]:
        load.wait()

    for h in range(H):
        cols = slice(h * D, (h + 1) * D)
        prod = g[:, cols].astype(F32) * o[:, cols].astype(F32)
        total = jnp.sum(prod, axis=1, keepdims=True) * factor
        delta[h] = jnp.broadcast_to(total, (S, D))
        line = jnp.broadcast_to(lse[h:h + 1, :] * LOG2E, (D, S))
        level[h] = line.T
        qt[h] = q[:, cols].T
        gt[h] = g[:, cols].T
    dqt[...] = jnp.zeros_like(dqt)
    own_stripe = stripe[me]

    cols_ = lax.broadcasted_iota(jnp.int32, (half, half), 1)
    diff = lax.broadcasted_iota(jnp.int32, (half, half), 0) - cols_

    def rows(i):
        return slice(i * half, (i + 1) * half)

    def wide(a):
        return jnp.concatenate([a] * (half // D), axis=1)

    def pair(slot, least, k, h0):
        units = [(h, r, w) for h in (h0, h0 + 1) for r, w in QUADS]
        open_ = diff >= least
        ks = [kv[slot, rows(w), :D] for w in range(2)]
        vs = [kv[slot, rows(w), D:] for w in range(2)]
        dk, dv, dq_part = {}, {}, {}

        def products(unit):
            h, r, w = unit
            cols = slice(h * D, (h + 1) * D)
            return dot(q[rows(r), cols], ks[w], 1, 1), dot(g[rows(r), cols], vs[w], 1, 1)

        def add(sums, key, term):
            sums[key] = sums[key] + term if key in sums else term

        def use(unit, score, weight):
            h, r, w = unit
            p = jnp.exp2(score * (factor * LOG2E) - wide(level[h, rows(r)]))
            if r == w:
                p = jnp.where(open_, p, 0.0)
            d = (p * (weight * factor - wide(delta[h, rows(r)]))).astype(BF16)
            add(dv, w, dot(gt[h, :, rows(r)], p.astype(BF16), 1, 0))
            add(dk, w, dot(qt[h, :, rows(r)], d, 1, 0))
            add(dq_part, (h, r), dot(d, ks[w], 1, 0))
            if r == w:
                dqt[h, rows(r)] += dq_part[h, r]

        waiting = []
        for unit in units:
            waiting.append((unit, products(unit)))
            if len(waiting) > LAG:
                unit, found = waiting.pop(0)
                use(unit, *found)
        for unit, found in waiting:
            use(unit, *found)
        for w in range(2):
            for m, total in enumerate((dk[w], dv[w])):
                if h0:
                    total = total + acc[k, w, m * D:(m + 1) * D, :]
                acc[k, w, m * D:(m + 1) * D, :] = total

    def near(i):
        return B(i), base - GROUP + i

    def side(i):
        return A(i), base + i - jnp.where(i > j, 2 * GROUP, 0)

    def compute(block, k, between):
        slot, source = block
        source = lax.rem(source + n, n)
        least = jnp.where(stripe[source] <= own_stripe, 0, 1)
        for h0 in range(0, H, 2):
            pair(slot, least, k, h0)
            if h0 == 0:
                between()

    def part_copies(kind):
        res = []
        if kind == SIDE:
            res.append(remote(part.at[kind, y], rx.at[kind, 0],
                              p_send.at[kind, 0], p_recv.at[kind, 0], (at(2), y)))
        to = at(2) if kind == SIDE else me
        res.append(remote(part.at[kind, 1 - y], rx.at[kind, 1],
                          p_send.at[kind, 1], p_recv.at[kind, 1], (to, 1 - y)))
        return res

    def send_part(kind):
        for copy in part_copies(kind):
            copy.start()

    def give(p):
        return remote(lend.at[p], take.at[p], d_send.at[p], d_recv.at[p], (at(1), y))

    def lend_out(p):
        lend[p] = acc[2 * p + 1 + c].astype(BF16)
        give(p).start()

    def join(p):
        give(p).wait_recv()
        part[NEAR + p] = (acc[2 * p + 2 - c] + take[p].astype(F32)).astype(BF16)
        send_part(NEAR + p)

    z_copies = [
        remote(zs.at[m], fin.at[m], z_send.at[m], z_recv.at[m], (to, y))
        for m, to in enumerate((plane(-1), owner(2), owner(1)))
    ]

    def forward(m, *kinds):
        total = arrived_part(kinds[0])
        for kind in kinds[1:]:
            total = total + arrived_part(kind)
        zs[m] = total.astype(BF16)
        z_copies[m].start()

    def arrived_part(kind):
        def get(m):
            remote(rx.at[kind, m], rx.at[kind, m], p_send.at[0, 0], p_recv.at[kind, m],
                   (at(1), y)).wait_recv()
            return rx[kind, m].astype(F32)

        first = part[kind, y].astype(F32) if kind != SIDE else get(0)
        return first + get(1)

    i_odd, i_even = 2 * x + 1, 2 * x
    o_odd, o_even = 3 - 2 * x, 2 - 2 * x

    on(0, up_b.start)
    on(1, side_own)

    def either(at0, at1):
        return (1 - c) * at0 + c * at1

    compute(side(j), 0, lambda: None)
    part[OWN] = acc[0].astype(BF16)
    on(1, spread_b, lambda: kv_arrived(A(mate(1))))
    on(0, lambda: kv_arrived(B(mate(1))))

    def step1():
        send_part(OWN)
        on(0, spread_b)

    compute(near(i_odd), 1, step1)
    on(0, lambda: lend_out(0))

    even, own_side = near(i_even), side(mate(1))
    compute(tuple(map(either, even, own_side)), either(2, 7), lambda: None)
    on(0, lambda: kv_arrived(A(mate(1))))
    on(1, pass_c, lambda: kv_arrived(B(mate(1))))

    def step3():
        on(0, pass_c)
        on(1, lambda: join(0))

    compute(tuple(map(either, own_side, even)), either(7, 2), step3)
    part[MATE] = acc[7].astype(BF16)
    on(0, lambda: kv_arrived(B(mate(3))))
    on(1, lambda: lend_out(0), relay_b)

    def step4():
        send_part(MATE)
        on(0, relay_b, lambda: join(0))

    compute(near(o_odd), 3, step4)
    on(0, lambda: lend_out(1))
    on(1, lambda: kv_arrived(B(mate(3))))

    def step5():
        on(1, relay_a, lambda: join(1))

    compute(near(o_even), 4, step5)
    on(1, lambda: lend_out(1))
    on(0, lambda: kv_arrived(A(mate(3))))

    def step6():
        on(0, relay_a, lambda: join(1))

    compute(side(o_odd), 5, step6)
    on(0, lambda: lend_out(2))
    on(1, lambda: kv_arrived(A(mate(3))))

    def step7():
        on(1, lambda: join(2))
        forward(2, MATE)

    compute(side(o_even), 6, step7)
    on(1, lambda: lend_out(2))

    for h in range(H):
        dq_out[:, h * D:(h + 1) * D] = dqt[h].astype(BF16)
    on(0, lambda: join(2))
    forward(0, NEAR, SIDE)
    forward(1, FAR)

    mine = arrived_part(OWN)
    for copy, m in zip(z_copies, range(3)):
        copy.wait_recv()
        mine = mine + fin[m].astype(F32)
    dk_out[...] = mine[:D].T.astype(BF16)
    dv_out[...] = mine[D:].T.astype(BF16)

    for copy in [up_b, own[1], own[2], b_out[1], b_out[2], b_relay, a_relay]:
        copy.wait_send()
    pl.when(j > 0)(up_c.wait_send)
    for kind in range(5):
        for copy in part_copies(kind):
            copy.wait_send()
    for p in range(PAIRS):
        give(p).wait_send()
    for copy in z_copies:
        copy.wait_send()


def emit(*refs):
    copies = [pltpu.make_async_copy(refs[m], refs[3 + m], refs[6].at[m]) for m in range(3)]
    for copy in copies:
        copy.start()
    for copy in copies:
        copy.wait()


def shards(n, query, key_rows, value_rows, output, grad_output, log_norm, stripe):
    S, W = query.shape
    D = key_rows.shape[1]
    H = W // D
    half = S // 2
    any_ = pl.BlockSpec(memory_space=pl.ANY)
    vm = pl.BlockSpec(memory_space=pltpu.VMEM)
    dma = pltpu.SemaphoreType.DMA
    arrays = (stripe, query, key_rows, value_rows, output, grad_output, log_norm)
    found = pl.pallas_call(
        functools.partial(kernel, n),
        out_shape=(
            jax.ShapeDtypeStruct((S, W), BF16),
            jax.ShapeDtypeStruct((half, D), BF16),
            jax.ShapeDtypeStruct((half, D), BF16),
        ),
        in_specs=[pl.BlockSpec(memory_space=pltpu.HBM)] * 7,
        out_specs=(vm, vm, vm),
        scratch_shapes=[
            pltpu.SMEM(stripe.shape, jnp.int32),
            pltpu.VMEM((S, W), BF16),
            pltpu.VMEM((S, W), BF16),
            pltpu.VMEM((S, W), BF16),
            pltpu.VMEM((H, S), F32),
            pltpu.VMEM((H, S, D), F32),
            pltpu.VMEM((H, S, D), F32),
            pltpu.VMEM((H, D, S), BF16),
            pltpu.VMEM((H, D, S), BF16),
            pltpu.VMEM((2 * GROUP + 1, S, 2 * D), BF16),
            pltpu.VMEM((H, S, D), F32),
            pltpu.VMEM((WINDOW, 2, 2 * D, half), F32),
            pltpu.VMEM((PAIRS, 2, 2 * D, half), BF16),
            pltpu.VMEM((PAIRS, 2, 2 * D, half), BF16),
            pltpu.VMEM((5, 2, 2 * D, half), BF16),
            pltpu.VMEM((5, 2, 2 * D, half), BF16),
            pltpu.VMEM((3, 2 * D, half), BF16),
            pltpu.VMEM((3, 2 * D, half), BF16),
            dma((7,)),
            dma((8,)),
            dma((2 * GROUP + 1,)),
            dma((PAIRS,)),
            dma((PAIRS,)),
            dma((5, 2)),
            dma((5, 2)),
            dma((3,)),
            dma((3,)),
        ],
        compiler_params=pltpu.CompilerParams(
            collective_id=0, has_side_effects=True, vmem_limit_bytes=33554432
        ),
        name="window_backward",
    )(*(pltpu.with_memory_space_constraint(a, pltpu.HBM) for a in arrays))
    return pl.pallas_call(
        emit,
        out_shape=tuple(jax.ShapeDtypeStruct(a.shape, a.dtype) for a in found),
        in_specs=[vm] * 3,
        out_specs=(any_,) * 3,
        scratch_shapes=[dma((3,))],
        compiler_params=pltpu.CompilerParams(vmem_limit_bytes=1 << 22),
        name="emit",
    )(*found)


def solution(mesh):
    placed = (
        P("seq", "head"),
        P("seq", None),
        P("seq", None),
        P("seq", "head"),
        P("seq", "head"),
        P("head", "seq"),
        P(),
    )
    return jax.shard_map(
        functools.partial(shards, mesh.shape["seq"]),
        mesh=mesh,
        in_specs=placed,
        out_specs=(P("seq", "head"), P(("seq", "head"), None), P(("seq", "head"), None)),
        check_vma=False,
    )
```
